768 devices in a mesh: head: 2 (over core), seq: 48 (over y_hi, z), mp: 8 (over x, y_lo).
Axes of the slice: x: 4, y: 8 (y_hi: 4, y_lo: 2; y = y_hi * 2 + y_lo), z: 12, core: 2. Of those that a mesh axis runs over, the one named last changes fastest.
Arguments:
- trunk: bfloat16 [768, 8192], P('seq', 'mp'), may hold values from -6 to 6
- branch: bfloat16 [2, 768, 8192], P('head', 'seq', 'mp'), may hold values from -6 to 6
- unembed: bfloat16 [18432, 8192], P('seq', 'mp'), may hold values from -0.09375 to 0.09375
- targets: int32 [2, 768], P('head'), may hold values from 0 to 18431
- loss_grad: float32 [2, 768], P('head'), may hold values from 0.25 to 4
Outputs:
- d_branch: bfloat16 [2, 768, 8192], P('head', 'seq', 'mp')
- d_trunk: bfloat16 [768, 8192], P('seq', 'mp')
- d_unembed: float32 [18432, 8192], P('seq', 'mp')
The draws below stay inside these ranges and needn't reach their ends.
All inputs are finite; a program needn't handle non-finite values.
Results may differ from the reference program's by a relative error of at most 0.0051.
Values may be sent and summed in bfloat16 or wider, within the bound.
A program may use at most 32 MiB of HBM per device.

```python
import math
import jax
import jax.numpy as jnp

D = 8192
V = 18432
TOKENS = 768
HEADS = 2


def plant(array, key, low, high):
    longest = array.shape.index(max(array.shape))
    spots = []
    for shift in (0, 1):
        where = [jax.random.randint(jax.random.fold_in(key, axis), (), 0, length) for axis, length in enumerate(array.shape)]
        where[longest] = (where[longest] + shift) % array.shape[longest]
        spots.append(tuple(where))
    return array.at[spots[0]].set(low).at[spots[1]].set(high)


def steps_of(key, extent, pieces, least, largest):
    def one(axis_at, parts):
        draws = jax.random.uniform(jax.random.fold_in(jax.random.fold_in(key, 6), axis_at), (parts,), jnp.float32, least / len(pieces), largest / len(pieces))
        return jnp.repeat(jnp.exp(draws), extent[axis_at] // parts).reshape((-1,) + (1,) * (len(extent) - axis_at - 1))

    gain = one(*pieces[0])
    for cut in pieces[1:]:
        gain = gain * one(*cut)
    return gain


def noise(own_key, shape, width, most, cuts=(), kind=jnp.bfloat16):
    values = jax.random.normal(own_key, shape, jnp.float32) * width
    if len(cuts) > 0:
        values = steps_of(own_key, shape, cuts, -0.22, 0.18) * values
    return jnp.clip(values, min=-most, max=most).astype(kind)


def setup_inputs(seed: int = 0) -> dict:
    key_of = jax.random.split(jax.random.key(seed), 6)
    return {
        "trunk": noise(key_of[0], (TOKENS, D), 1.0, 6.0, ((0, 48), (1, 8))),
        "branch": noise(key_of[1], (HEADS, TOKENS, D), 1.0, 6.0, ((0, 2), (1, 48), (2, 8))),
        "unembed": noise(key_of[2], (V, D), (D * 4 // 9) ** -0.5, 0.09375, ((0, 48), (1, 8))),
        "targets": plant(jax.random.randint(key_of[3], (HEADS, TOKENS), 0, V), jax.random.fold_in(key_of[3], 1), 0, V - 1).astype(jnp.int32),
        "loss_grad": jnp.clip(jnp.exp(math.log(4.0) - 2.7725887 * jax.random.uniform(key_of[4], (HEADS, TOKENS), jnp.float32) ** steps_of(key_of[4], (HEADS, TOKENS), ((0, 2),), -0.2, 0.2)), 0.25, 4.0),
    }


soft_cap = 30.0


def reference(trunk, branch, unembed, targets, loss_grad):
    vocab_ids = jnp.arange(V, dtype=jnp.int32)
    grads = []
    trunk_grad = jnp.zeros((TOKENS, D), jnp.float32)
    unembed_grad = jnp.zeros((V, D), jnp.float32)
    for which in range(HEADS):
        hidden = (trunk.astype(jnp.float32) + branch[which].astype(jnp.float32)).astype(jnp.bfloat16)
        scores = jnp.dot(hidden, unembed.T, preferred_element_type=jnp.float32)
        squashed = jnp.tanh(scores / soft_cap)
        exponent = jnp.exp(soft_cap * squashed)
        totals = jnp.sum(exponent, axis=1)
        onehot = (targets[which][:, None] == vocab_ids[None, :]).astype(jnp.float32)
        slope = loss_grad[which][:, None] * (exponent / totals[:, None] - onehot) * (1.0 - squashed * squashed)
        grad_logits = slope.astype(jnp.bfloat16)
        row_grad = jnp.dot(grad_logits, unembed, preferred_element_type=jnp.float32)
        grads.append(row_grad.astype(jnp.bfloat16))
        trunk_grad = trunk_grad + row_grad
        unembed_grad = unembed_grad + jnp.dot(grad_logits.T, hidden, preferred_element_type=jnp.float32)
    return jnp.stack(grads), trunk_grad.astype(jnp.bfloat16), unembed_grad
```

```python
import functools

import jax
import jax.numpy as jnp
from jax import lax
from jax.experimental import pallas as pl
from jax.experimental.pallas import tpu as pltpu
from jax.sharding import Mesh
from jax.sharding import PartitionSpec as P

MESH = pl.DeviceIdType.MESH
SEQ = ("yh", "z")
MP = ("x", "yl")
F32, BF16 = jnp.float32, jnp.bfloat16

soft_cap = 30.0


def reach(n, j):
    far, near = n // 2, (n - 1) // 2
    return (far, near) if j % 2 == 0 else (near, far)


def step_kernel(
    sizes,
    trunk_ref,
    branch_ref,
    unembed_hbm,
    targets_ref,
    loss_grad_ref,
    d_branch_ref,
    d_trunk_ref,
    d_unembed_ref,
    unembed_ref,
    hid,
    part_out,
    part_in,
    tot_mp,
    tot_z,
    tot_y,
    tot_out,
    grads,
    grads_t,
    rows_part,
    rs_out,
    rs_in,
    y_out,
    y_in,
    own_rows,
    head_rows,
    own_weight,
    head_weight,
    local_sem,
    y_sems,
    ring_sems,
    part_sems,
    tot_mp_sems,
    tot_z_sems,
    tot_y_sems,
    grad_sems,
    rs_sems,
    yr_sems,
    head_sems,
):
    NH, NY, NZ, NX, NL = sizes
    NM = NX * NL
    head = lax.axis_index("head")
    yh, z = lax.axis_index("yh"), lax.axis_index("z")
    x, yl = lax.axis_index("x"), lax.axis_index("yl")
    block_rows = unembed_ref.shape[0]
    share = block_rows // NM
    rows = NY * NZ * hid.shape[1]
    RB, DS = hid.shape[1], hid.shape[2]

    def at_y(d):
        return lax.rem(yh + (d + NY), NY)

    def at_z(d):
        return lax.rem(z + (d + NZ), NZ)

    def mp_peer(d):
        dx, dl = d // NL, d % NL
        return lax.rem(x + dx, NX), lax.rem(yl + dl, NL)

    def mp_from(d):
        dx, dl = d // NL, d % NL
        return lax.rem(x + (NX - dx), NX), lax.rem(yl + (NL - dl), NL)

    def block(a, b):
        return a * NZ + b

    sent = []

    def copy(src, dst, sems, at, device):
        return pltpu.make_async_remote_copy(
            src_ref=src,
            dst_ref=dst,
            send_sem=sems.at[(0, *at)],
            recv_sem=sems.at[(1, *at)],
            device_id=device,
            device_id_type=MESH,
        )

    def send(*args):
        c = copy(*args)
        c.start()
        sent.append(c)

    load_unembed = pltpu.make_async_copy(unembed_hbm, unembed_ref, local_sem)
    load_unembed.start()

    barrier = pltpu.get_barrier_semaphore()
    peers = [{"yh": at_y(d)} for d in range(1, NY)]
    peers += [{"z": at_z(1)}, {"z": at_z(-1)}]
    for d in range(1, NM):
        px, pyl = mp_peer(d)
        peers.append({"x": px, "yl": pyl})
    peers.append({"head": 1 - head})
    for device in peers:
        pl.semaphore_signal(barrier, inc=1, device_id=device, device_id_type=MESH)

    me = block(yh, z)
    hid[me] = (trunk_ref[...].astype(F32) + branch_ref[0].astype(F32)).astype(BF16)
    pl.semaphore_wait(barrier, len(peers))

    ring = ({"z": at_z(1)}, {"z": at_z(-1)})

    def ring_send(way, k, j):
        origin = block(at_y(-j), at_z(-k if way == 0 else k))
        send(hid.at[origin], hid.at[origin], ring_sems, (way, k, j), ring[way])

    def ring_wait(way, k, j):
        origin = block(at_y(-j), at_z(-k if way == 0 else k))
        copy(hid.at[origin], hid.at[origin], ring_sems, (way, k - 1, j), ring[way]).wait_recv()

    for d in range(1, NY):
        send(hid.at[me], hid.at[me], y_sems, (d,), {"yh": at_y(d)})
    order = [j for j in (0, 1, 3, 2) if j < NY]
    for j in order:
        if j:
            origin = block(at_y(-j), z)
            copy(hid.at[origin], hid.at[origin], y_sems, (j,), {"yh": at_y(j)}).wait_recv()
        for way in (0, 1):
            if reach(NZ, j)[way] > 0:
                ring_send(way, 0, j)
    for k in range(1, NZ // 2 + 1):
        for j in order:
            for way in (0, 1):
                limit = reach(NZ, j)[way]
                if k <= limit:
                    ring_wait(way, k, j)
                    if k < limit:
                        ring_send(way, k, j)

    load_unembed.wait()
    lanes = min(256, rows)
    for c in range(rows // lanes):
        chunk = hid[c * (lanes // RB) : (c + 1) * (lanes // RB)].reshape(lanes, DS)
        partial = lax.dot_general(
            unembed_ref[...], chunk, (((1,), (1,)), ((), ())), preferred_element_type=F32
        )
        part_out[:, :, c * lanes : (c + 1) * lanes] = partial.astype(BF16).reshape(NM, share, lanes)
    mine = x * NL + yl
    for d in range(1, NM):
        px, pyl = mp_peer(d)
        send(part_out.at[px * NL + pyl], part_in.at[d], part_sems, (d,), {"x": px, "yl": pyl})
    scores = part_out[mine].astype(F32)
    for d in range(1, NM):
        px, pyl = mp_peer(d)
        copy(part_in.at[d], part_in.at[d], part_sems, (d,), {"x": px, "yl": pyl}).wait_recv()
        scores = scores + part_in[d].astype(F32)
    squashed = jnp.tanh(scores / soft_cap)
    exponent = jnp.exp(soft_cap * squashed)

    total = jnp.sum(exponent, axis=0, keepdims=True)
    tot_out[0] = total
    for d in range(1, NM):
        px, pyl = mp_peer(d)
        send(tot_out.at[0], tot_mp.at[d], tot_mp_sems, (d,), {"x": px, "yl": pyl})
    for d in range(1, NM):
        px, pyl = mp_peer(d)
        copy(tot_mp.at[d], tot_mp.at[d], tot_mp_sems, (d,), {"x": px, "yl": pyl}).wait_recv()
        total = total + tot_mp[d]
    tot_out[1] = total
    for d in range(1, NZ):
        send(tot_out.at[1], tot_z.at[d], tot_z_sems, (d,), {"z": at_z(d)})
    for d in range(1, NZ):
        copy(tot_z.at[d], tot_z.at[d], tot_z_sems, (d,), {"z": at_z(d)}).wait_recv()
        total = total + tot_z[d]
    tot_out[2] = total
    for d in range(1, NY):
        send(tot_out.at[2], tot_y.at[d], tot_y_sems, (d,), {"yh": at_y(d)})
    for d in range(1, NY):
        copy(tot_y.at[d], tot_y.at[d], tot_y_sems, (d,), {"yh": at_y(d)}).wait_recv()
        total = total + tot_y[d]

    first_vocab = me * block_rows + mine * share
    vocab_ids = first_vocab + lax.broadcasted_iota(jnp.int32, (share, rows), 0)
    onehot = (vocab_ids == targets_ref[...]).astype(F32)
    slope = loss_grad_ref[...] * (exponent / total - onehot) * (1.0 - squashed * squashed)
    grads[mine] = slope.astype(BF16)
    for d in range(1, NM):
        px, pyl = mp_peer(d)
        send(grads.at[mine], grads.at[mine], grad_sems, (d,), {"x": px, "yl": pyl})
    for d in range(1, NM):
        px, pyl = mp_from(d)
        origin = px * NL + pyl
        copy(grads.at[origin], grads.at[origin], grad_sems, (d,), {"x": px, "yl": pyl}).wait_recv()

    for c in range(rows // 128):
        piece = grads[:, :, c * 128 : (c + 1) * 128].reshape(block_rows, 128)
        grads_t[c * 128 : (c + 1) * 128, :] = piece.T
    for c in range(rows // lanes):
        partial = jnp.dot(
            grads_t[c * lanes : (c + 1) * lanes, :], unembed_ref[...], preferred_element_type=F32
        )
        rows_part[c * (lanes // RB) : (c + 1) * (lanes // RB)] = partial.reshape(lanes // RB, RB, DS)

    back = [j for j in (2, 1, 3, 0) if j < NY]

    def rs_step(way, i, j):
        limit = reach(NZ, j)[way]
        ahead = limit - i
        target = block(at_y(j), at_z(ahead if way == 0 else -ahead))
        value = rows_part[target]
        if i > 0:
            copy(
                rs_in.at[way, i - 1, j], rs_in.at[way, i - 1, j], rs_sems, (way, i - 1, j), ring[way]
            ).wait_recv()
            value = value + rs_in[way, i - 1, j].astype(F32)
        if i < limit:
            rs_out[way, i, j] = value.astype(BF16)
            send(rs_out.at[way, i, j], rs_in.at[way, i, j], rs_sems, (way, i, j), ring[way])

    for j in back:
        for way in (0, 1):
            if reach(NZ, j)[way] > 0:
                rs_step(way, 0, j)

    all_grads = grads[...].reshape(block_rows, rows)
    cols = min(256, DS)
    for c in range(DS // cols):
        own_weight[:, c * cols : (c + 1) * cols] = jnp.dot(
            all_grads,
            hid[:, :, c * cols : (c + 1) * cols].reshape(rows, cols),
            preferred_element_type=F32,
        )
    send(own_weight, head_weight, head_sems, (0,), {"head": 1 - head})

    for i in range(1, NZ // 2 + 1):
        for j in back:
            for way in (0, 1):
                if i < reach(NZ, j)[way]:
                    rs_step(way, i, j)
    for j in back:
        value = rows_part[block(at_y(j), z)]
        for way in (0, 1):
            limit = reach(NZ, j)[way]
            if limit > 0:
                slot = rs_in.at[way, limit - 1, j]
                copy(slot, slot, rs_sems, (way, limit - 1, j), ring[way]).wait_recv()
                value = value + rs_in[way, limit - 1, j].astype(F32)
        if j:
            y_out[j] = value.astype(BF16)
            send(y_out.at[j], y_in.at[j], yr_sems, (j,), {"yh": at_y(j)})
        else:
            row_grad = value
    copy(own_weight, head_weight, head_sems, (0,), {"head": 1 - head}).wait_recv()
    d_unembed_ref[...] = own_weight[...] + head_weight[...]
    for j in range(1, NY):
        copy(y_in.at[j], y_in.at[j], yr_sems, (j,), {"yh": at_y(j)}).wait_recv()
        row_grad = row_grad + y_in[j].astype(F32)
    own_rows[...] = row_grad
    send(own_rows, head_rows, head_sems, (1,), {"head": 1 - head})
    d_branch_ref[0] = row_grad.astype(BF16)
    copy(own_rows, head_rows, head_sems, (1,), {"head": 1 - head}).wait_recv()
    d_trunk_ref[...] = (row_grad + head_rows[...]).astype(BF16)
    for c in sent:
        c.wait_send()


def shards(sizes, trunk, branch, unembed, targets, loss_grad):
    NH, NY, NZ, NX, NL = sizes
    NM = NX * NL
    RB, DS = trunk.shape
    VB = unembed.shape[0]
    share, rows = VB // NM, NY * NZ * RB
    steps = NZ // 2
    sem = pltpu.SemaphoreType.DMA
    vmem = pl.BlockSpec(memory_space=pltpu.VMEM)
    return pl.pallas_call(
        functools.partial(step_kernel, sizes),
        out_shape=(
            jax.ShapeDtypeStruct((1, RB, DS), BF16),
            jax.ShapeDtypeStruct((RB, DS), BF16),
            jax.ShapeDtypeStruct((VB, DS), F32),
        ),
        in_specs=[vmem, vmem, pl.BlockSpec(memory_space=pl.ANY), vmem, vmem],
        out_specs=(vmem, vmem, vmem),
        scratch_shapes=[
            pltpu.VMEM((VB, DS), BF16),
            pltpu.VMEM((NY * NZ, RB, DS), BF16),
            pltpu.VMEM((NM, share, rows), BF16),
            pltpu.VMEM((NM, share, rows), BF16),
            pltpu.VMEM((NM, 1, rows), F32),
            pltpu.VMEM((NZ, 1, rows), F32),
            pltpu.VMEM((NY, 1, rows), F32),
            pltpu.VMEM((3, 1, rows), F32),
            pltpu.VMEM((NM, share, rows), BF16),
            pltpu.VMEM((rows, VB), BF16),
            pltpu.VMEM((NY * NZ, RB, DS), F32),
            pltpu.VMEM((2, steps, NY, RB, DS), BF16),
            pltpu.VMEM((2, steps, NY, RB, DS), BF16),
            pltpu.VMEM((NY, RB, DS), BF16),
            pltpu.VMEM((NY, RB, DS), BF16),
            pltpu.VMEM((RB, DS), F32),
            pltpu.VMEM((RB, DS), F32),
            pltpu.VMEM((VB, DS), F32),
            pltpu.VMEM((VB, DS), F32),
            sem,
            sem((2, NY)),
            sem((2, 2, steps, NY)),
            sem((2, NM)),
            sem((2, NM)),
            sem((2, NZ)),
            sem((2, NY)),
            sem((2, NM)),
            sem((2, 2, steps, NY)),
            sem((2, NY)),
            sem((2, 2)),
        ],
        compiler_params=pltpu.CompilerParams(
            collective_id=0, has_side_effects=True, vmem_limit_bytes=48 * 1024 * 1024
        ),
    )(trunk, branch, unembed, targets, loss_grad)


def solution(mesh, sizes=(2, 4, 12, 4, 2)):
    split = Mesh(mesh.devices.reshape(sizes), ("head", "yh", "z", "x", "yl"))
    return jax.shard_map(
        functools.partial(shards, sizes),
        mesh=split,
        in_specs=(P(SEQ, MP), P("head", SEQ, MP), P(SEQ, MP), P("head", None), P("head", None)),
        out_specs=(P("head", SEQ, MP), P(SEQ, MP), P(SEQ, MP)),
        check_vma=False,
    )
```
